32 devices in a mesh: dp: 8 (over z, y), sp: 4 (over x, core).
Axes of the slice: x: 2, y: 2, z: 4, core: 2. Of those that a mesh axis runs over, the one named last changes fastest.
Arguments:
- latents: bfloat16 [24, 48, 96, 384], P('dp', 'sp')
- t_mod: float32 [24, 6, 384], P('dp')
- t_mod_zero: float32 [24, 6, 384], P('dp')
- frame_mask: int32 [24, 48], P('dp')
- captions: bfloat16 [24, 120, 384], P('dp')
- caption_len: int32 [24], P('dp')
- w_qkv: bfloat16 [2, 384, 3, 6, 64], replicated
- w_out: bfloat16 [2, 6, 64, 384], replicated
- w_cross_q: bfloat16 [2, 384, 6, 64], replicated
- w_cross_kv: bfloat16 [2, 384, 2, 6, 64], replicated
- w_cross_out: bfloat16 [2, 6, 64, 384], replicated
- w_mlp_in: bfloat16 [2, 384, 1536], replicated
- w_mlp_out: bfloat16 [2, 1536, 384], replicated
- mod_table: float32 [2, 6, 384], replicated
- grad_out: bfloat16 [24, 48, 96, 384], P('dp', 'sp')
Outputs:
- output 1: bfloat16 [24, 48, 96, 384], P('dp', 'sp')
- output 2: float32 [2, 384, 3, 6, 64], replicated
- output 3: float32 [2, 6, 64, 384], replicated
- output 4: float32 [2, 384, 6, 64], replicated
- output 5: float32 [2, 384, 2, 6, 64], replicated
- output 6: float32 [2, 6, 64, 384], replicated
- output 7: float32 [2, 384, 1536], replicated
- output 8: float32 [2, 1536, 384], replicated
- output 9: float32 [2, 6, 384], replicated
All inputs are finite; a program needn't handle non-finite values.
Results may differ from the reference program's by a relative error of at most 0.02.
Values are sent between devices in bfloat16 or wider.
A program may use at most 1 GiB of HBM per device.

```python
import jax
import jax.numpy as jnp
from jax import lax

WIDTH = 384
NUM_HEADS = 6
HEAD_DIM = 64
MLP_DIM = 1536
TEXT_LEN = 120
BATCH = 24
FRAMES = 48
SPATIAL = 96


def setup_inputs(seed: int = 0) -> dict:
    keys = jax.random.split(jax.random.key(seed), 16)

    def normal(one_key, shape, scale):
        return scale * jax.random.normal(one_key, shape, jnp.float32)

    perm_keys = jax.random.split(keys[3], BATCH)
    ranks = jax.vmap(lambda one_key: jax.random.permutation(one_key, FRAMES))(perm_keys)
    cond_low = max(1, (FRAMES + 4) // 5)
    cond_high = max(cond_low, FRAMES // 2)
    cond_count = jax.random.randint(keys[4], (BATCH, 1), cond_low, cond_high + 1, dtype=jnp.int32)
    frame_mask = (ranks >= cond_count).astype(jnp.int32)
    caption_len = jax.random.randint(keys[5], (BATCH,), 1, TEXT_LEN + 1, dtype=jnp.int32).at[0].set(TEXT_LEN)
    in_scale = WIDTH ** -0.5
    return {
        'latents': normal(keys[0], (BATCH, FRAMES, SPATIAL, WIDTH), 1.0).astype(jnp.bfloat16),
        't_mod': normal(keys[1], (BATCH, 6, WIDTH), 0.5),
        't_mod_zero': normal(keys[2], (BATCH, 6, WIDTH), 0.5),
        'frame_mask': frame_mask,
        'captions': normal(keys[6], (BATCH, TEXT_LEN, WIDTH), 1.0).astype(jnp.bfloat16),
        'caption_len': caption_len,
        'w_qkv': normal(keys[7], (2, WIDTH, 3, NUM_HEADS, HEAD_DIM), in_scale).astype(jnp.bfloat16),
        'w_out': normal(keys[8], (2, NUM_HEADS, HEAD_DIM, WIDTH), in_scale).astype(jnp.bfloat16),
        'w_cross_q': normal(keys[9], (2, WIDTH, NUM_HEADS, HEAD_DIM), in_scale).astype(jnp.bfloat16),
        'w_cross_kv': normal(keys[10], (2, WIDTH, 2, NUM_HEADS, HEAD_DIM), in_scale).astype(jnp.bfloat16),
        'w_cross_out': normal(keys[11], (2, NUM_HEADS, HEAD_DIM, WIDTH), in_scale).astype(jnp.bfloat16),
        'w_mlp_in': normal(keys[12], (2, WIDTH, MLP_DIM), in_scale).astype(jnp.bfloat16),
        'w_mlp_out': normal(keys[13], (2, MLP_DIM, WIDTH), MLP_DIM ** -0.5).astype(jnp.bfloat16),
        'mod_table': normal(keys[14], (2, 6, WIDTH), 0.4),
        'grad_out': normal(keys[15], (BATCH, FRAMES, SPATIAL, WIDTH), 1.0).astype(jnp.bfloat16),
    }


def layer_norm(hidden_in):
    centered = hidden_in - jnp.mean(hidden_in, axis=-1, keepdims=True)
    return centered * lax.rsqrt(jnp.mean(jnp.square(centered), axis=-1, keepdims=True) + 1e-6)


def rms_heads(head_vec):
    return head_vec * lax.rsqrt(jnp.mean(jnp.square(head_vec), axis=-1, keepdims=True) + 1e-6)


def rotary(head_vec):
    half = head_vec.shape[-1] // 2
    inv_freq = 10000.0 ** (-jnp.arange(half, dtype=jnp.float32) / half)
    angle = jnp.arange(head_vec.shape[0], dtype=jnp.float32)[:, None] * inv_freq[None, :]
    cosine = jnp.cos(angle)[:, None, None, :]
    sine = jnp.sin(angle)[:, None, None, :]
    first = head_vec[..., :half]
    second = head_vec[..., half:]
    return jnp.concatenate([first * cosine - second * sine, first * sine + second * cosine], axis=-1)


def block(weight_set, latents, base, captions, caption_len, temporal):
    w_qkv, w_out, w_cross_q, w_cross_kv, w_cross_out, w_mlp_in, w_mlp_out, mod_table = weight_set
    n_frames = latents.shape[0]
    n_patch = latents.shape[1]
    mod_terms = (mod_table + base)[:, None]
    shift_att = mod_terms[:, :, 0]
    scale_att = mod_terms[:, :, 1]
    gate_att = mod_terms[:, :, 2]
    shift_mlp = mod_terms[:, :, 3]
    scale_mlp = mod_terms[:, :, 4]
    gate_mlp = mod_terms[:, :, 5]
    attn_scale = HEAD_DIM ** -0.5
    residual = latents.astype(jnp.float32)
    normed = (layer_norm(residual) * (1.0 + scale_att) + shift_att).astype(jnp.bfloat16)
    qkv_all = jnp.dot(normed.reshape(-1, WIDTH), w_qkv.reshape(WIDTH, -1), preferred_element_type=jnp.float32)
    qkv_all = qkv_all.reshape(n_frames, n_patch, 3, NUM_HEADS, HEAD_DIM)
    query = rms_heads(qkv_all[:, :, 0])
    keys = rms_heads(qkv_all[:, :, 1])
    values = qkv_all[:, :, 2].astype(jnp.bfloat16).astype(jnp.float32)
    if temporal:
        query = rotary(query)
        keys = rotary(keys)
        form_scores = 'qghe,kghe->ghqk'
        form_out = 'ghqk,kghe->qghe'
    else:
        form_scores = 'gqhe,gkhe->ghqk'
        form_out = 'ghqk,gkhe->gqhe'
    query = query.astype(jnp.bfloat16).astype(jnp.float32)
    keys = keys.astype(jnp.bfloat16).astype(jnp.float32)
    scores = jnp.einsum(form_scores, query, keys) * attn_scale
    attn_prob = jax.nn.softmax(scores, axis=-1).astype(jnp.bfloat16).astype(jnp.float32)
    heads_out = jnp.einsum(form_out, attn_prob, values).astype(jnp.bfloat16)
    attn_proj = jnp.dot(heads_out.reshape(-1, WIDTH), w_out.reshape(WIDTH, WIDTH), preferred_element_type=jnp.float32)
    residual = (residual + gate_att * attn_proj.reshape(n_frames, n_patch, WIDTH)).astype(jnp.bfloat16)
    cross_q = jnp.dot(residual.reshape(-1, WIDTH), w_cross_q.reshape(WIDTH, WIDTH), preferred_element_type=jnp.float32)
    cross_q = cross_q.astype(jnp.bfloat16).astype(jnp.float32).reshape(-1, NUM_HEADS, HEAD_DIM)
    cross_kv = jnp.dot(captions, w_cross_kv.reshape(WIDTH, -1), preferred_element_type=jnp.float32)
    cross_kv = cross_kv.astype(jnp.bfloat16).astype(jnp.float32).reshape(-1, 2, NUM_HEADS, HEAD_DIM)
    scores = jnp.einsum('nhe,mhe->hnm', cross_q, cross_kv[:, 0]) * attn_scale
    key_valid = jnp.arange(captions.shape[0])[None, None, :] < caption_len
    scores = jnp.where(key_valid, scores, -1e30)
    attn_prob = jax.nn.softmax(scores, axis=-1).astype(jnp.bfloat16).astype(jnp.float32)
    cross_heads = jnp.einsum('hnm,mhe->nhe', attn_prob, cross_kv[:, 1]).astype(jnp.bfloat16)
    cross_proj = jnp.dot(cross_heads.reshape(-1, WIDTH), w_cross_out.reshape(WIDTH, WIDTH), preferred_element_type=jnp.float32)
    residual = (residual.astype(jnp.float32) + cross_proj.reshape(n_frames, n_patch, WIDTH)).astype(jnp.bfloat16)
    residual = residual.astype(jnp.float32)
    normed = (layer_norm(residual) * (1.0 + scale_mlp) + shift_mlp).astype(jnp.bfloat16)
    hidden = jax.nn.gelu(jnp.dot(normed.reshape(-1, WIDTH), w_mlp_in, preferred_element_type=jnp.float32), approximate=True).astype(jnp.bfloat16)
    mlp_out = jnp.dot(hidden, w_mlp_out, preferred_element_type=jnp.float32)
    return (residual + gate_mlp * mlp_out.reshape(n_frames, n_patch, WIDTH)).astype(jnp.bfloat16)


def sample_forward(param_set, latents, base, captions, caption_len):
    first = tuple(param[0] for param in param_set)
    second = tuple(param[1] for param in param_set)
    middle = block(first, latents, base, captions, caption_len, False)
    return block(second, middle, base, captions, caption_len, True)


def reference(latents, t_mod, t_mod_zero, frame_mask, captions, caption_len, w_qkv, w_out, w_cross_q, w_cross_kv, w_cross_out, w_mlp_in, w_mlp_out, mod_table, grad_out):
    param_set = (w_qkv, w_out, w_cross_q, w_cross_kv, w_cross_out, w_mlp_in, w_mlp_out, mod_table)
    base = jnp.where(frame_mask[:, :, None, None] == 1, t_mod[:, None], t_mod_zero[:, None])

    def per_sample(carry, item):
        lat_in, base_in, cap_in, len_in, grad_in = item

        def forward(params_in, lat_arg):
            return sample_forward(params_in, lat_arg, base_in, cap_in, len_in)

        fwd_out, pullback = jax.vjp(forward, param_set, lat_in)
        grad_params, grad_lat = pullback(grad_in)
        carry = tuple(running + grad.astype(jnp.float32) for running, grad in zip(carry, grad_params))
        return carry, grad_lat

    zero_grads = tuple(jnp.zeros(param.shape, jnp.float32) for param in param_set)
    grads, grad_latents = lax.scan(per_sample, zero_grads, (latents, base, captions, caption_len, grad_out))
    return (grad_latents, grads[0], grads[1], grads[2], grads[3], grads[4], grads[5], grads[6], grads[7])
```

```python
import functools

import jax
import jax.numpy as jnp
from jax import lax
from jax.experimental import pallas as pl
from jax.experimental.pallas import tpu as pltpu
from jax.sharding import PartitionSpec as P

BF = jnp.bfloat16
F32 = jnp.float32
D = 384
HID = 1536
TILE = 384
GRP = 96
NG = TILE // GRP
TILES = 3
ROWS = TILE * TILES
CAP = 128
CH = 256
K0 = 0.7978845608028654
K1 = 0.044715
R_QKV, R_OUT, R_CQ, R_CKV, R_CO, R_MO, R_MOD, R_END = 0, 1152, 1536, 1920, 2688, 3072, 4608, 4656
VMEM_LIMIT = 66 * 1000 * 1000


def dnn(a, b):
    return lax.dot_general(a, b, (((1,), (0,)), ((), ())), preferred_element_type=F32)


def dnt(a, b):
    return lax.dot_general(a, b, (((1,), (1,)), ((), ())), preferred_element_type=F32)


def dtn(a, b):
    return lax.dot_general(a, b, (((0,), (0,)), ((), ())), preferred_element_type=F32)


def layer_norm(x):
    centered = x - jnp.mean(x, axis=-1, keepdims=True)
    rstd = lax.rsqrt(jnp.mean(centered * centered, axis=-1, keepdims=True) + 1e-6)
    return centered * rstd, rstd


def layer_norm_bwd(grad, normed, rstd):
    mean_g = jnp.mean(grad, axis=-1, keepdims=True)
    mean_gn = jnp.mean(grad * normed, axis=-1, keepdims=True)
    return rstd * (grad - mean_g - normed * mean_gn)


def rows8(x):
    return jnp.sum(x.reshape(x.shape[0] // 8, 8, x.shape[1]), axis=0)


def lane_low(rows):
    return lax.broadcasted_iota(jnp.int32, (rows, 128), 1) < 64


def head_sum_matrix():
    row = lax.broadcasted_iota(jnp.int32, (256, 128), 0)
    col = lax.broadcasted_iota(jnp.int32, (256, 128), 1)
    return jnp.where((row % 128) // 64 == col // 64, 1.0, 0.0).astype(BF)


def head_sum(x, ones):
    hi = x.astype(BF)
    lo = (x - hi.astype(F32)).astype(BF)
    return dnn(jnp.concatenate([hi, lo], axis=1), ones)


def swap_halves(x):
    lane = lax.broadcasted_iota(jnp.int32, x.shape, 1)
    return jnp.where(lane % 64 < 32, pltpu.roll(x, 96, 1), pltpu.roll(x, 32, 1))


def stack_heads(x, low, high):
    return jnp.concatenate([x * low, x * high], axis=0)


def pick_heads(x2, rows):
    return jnp.where(lane_low(rows), x2[:rows], x2[rows:])


def block_kernel(temporal, backward, len_ref, *refs):
    refs = list(refs)
    take = refs.pop
    x_ref = take(0)
    g_ref = take(0) if backward else None
    mods_ref, msk_ref, cap_ref = take(0), take(0), take(0)
    wqkv, wout, wcq, wckv, wco, win, wmo = [take(0) for _ in range(7)]
    if temporal:
        cos_ref, sin_ref, perm_ref = take(0), take(0), take(0)
    out_ref = take(0)
    if backward:
        acc_ref, accw_ref = take(0), take(0)
    qb_ref, vb_ref, kv_ref, m_ref = take(0), take(0), take(0), take(0)
    h_s, o_s, x1_s, oc_s, n_s = [take(0) for _ in range(5)]
    if backward:
        hid_s, dm_s, du_s, dx2_s, dqc_s, da_s, dqkv_s = [take(0) for _ in range(7)]
        qn_ref, rq_ref, ps_ref, pc_ref, a_ref, dn_ref, dkv_ref, do_ref, dqk_ref = [take(0) for _ in range(9)]

    s = pl.program_id(0)
    t = pl.program_id(1)
    r0 = pl.multiple_of(t * TILE, TILE) if backward else 0
    here = pl.ds(r0, TILE)
    lane_row = lax.broadcasted_iota(jnp.int32, (1, 128), 1)
    low = jnp.where(lane_row < 64, 1.0, 0.0).astype(BF)
    high = jnp.where(lane_row < 64, 0.0, 1.0).astype(BF)
    ones = head_sum_matrix()
    cond = msk_ref[0, 0] > 0.5

    def mod(index):
        return jnp.where(cond, mods_ref[0, index:index + 1, :], mods_ref[0, 8 + index:9 + index, :])

    if backward:
        @pl.when((s == 0) & (t == 0))
        def _():
            acc_ref[...] = jnp.zeros_like(acc_ref)
            accw_ref[...] = jnp.zeros_like(accw_ref)

    @pl.when(t == 0)
    def _():
        kv_ref[...] = dnt(cap_ref[0], wckv[0]).astype(BF)
        if backward:
            dkv_ref[...] = jnp.zeros_like(dkv_ref)

    def load_x():
        if temporal:
            return dnn(perm_ref[...], x_ref[...].reshape(TILE, D))
        return x_ref[...].reshape(TILE, D).astype(F32)

    normed, _ = layer_norm(load_x())
    h = (normed * (1.0 + mod(1)) + mod(0)).astype(BF)
    h_s[here, :] = h
    qkv = dnt(h, wqkv[0])
    for j in range(6):
        cols = slice(j * 128, (j + 1) * 128)
        raw = qkv[:, cols]
        inv = lax.rsqrt(head_sum(raw * raw, ones) * (1.0 / 64) + 1e-6)
        unit = raw * inv
        if backward:
            qn_ref[:, cols] = unit
            rq_ref[:, cols] = inv
        if temporal:
            unit = unit * cos_ref[...] + swap_halves(unit) * sin_ref[...]
        qb_ref[:, cols] = unit.astype(BF)
    vb_ref[...] = qkv[:, 2 * D:].astype(BF)

    if temporal:
        same = (lax.broadcasted_iota(jnp.int32, (2 * GRP, GRP), 0) // 48) % 2 == lax.broadcasted_iota(jnp.int32, (2 * GRP, GRP), 1) // 48

    def self_fwd(grp, carry):
        rows = pl.ds(pl.multiple_of(grp * GRP, GRP), GRP)
        for p in range(3):
            cols = slice(p * 128, (p + 1) * 128)
            kcols = slice(D + p * 128, D + (p + 1) * 128)
            q2 = stack_heads(qb_ref[rows, cols], low, high)
            e = jnp.exp(dnt(q2, qb_ref[rows, kcols]) * 0.125)
            if temporal:
                e = jnp.where(same, e, 0.0)
            prob = e * (1.0 / jnp.sum(e, axis=-1, keepdims=True))
            if backward:
                ps_ref[grp * 3 + p] = prob
            o2 = dnn(prob.astype(BF), vb_ref[rows, cols])
            o_s[pl.ds(pl.multiple_of(r0 + grp * GRP, GRP), GRP), cols] = pick_heads(o2, GRP).astype(BF)
        return carry

    lax.fori_loop(0, NG, self_fwd, 0)

    attn = dnn(o_s[here, :], wout[0])
    if backward:
        a_ref[...] = attn
    x1 = (load_x() + mod(2) * attn).astype(BF)
    x1_s[here, :] = x1

    qc = dnt(x1, wcq[0]).astype(BF)
    valid = lax.broadcasted_iota(jnp.int32, (2 * TILE, CAP), 1) < len_ref[s]
    for p in range(3):
        cols = slice(p * 128, (p + 1) * 128)
        q2 = stack_heads(qc[:, cols], low, high)
        sc = jnp.where(valid, dnt(q2, kv_ref[:, cols]) * 0.125, -1e30)
        e = jnp.exp(sc - jnp.max(sc, axis=-1, keepdims=True))
        prob = e * (1.0 / jnp.sum(e, axis=-1, keepdims=True))
        if backward:
            pc_ref[p] = prob
            dqc_s[here, cols] = qc[:, cols]
        o2 = dnn(prob.astype(BF), kv_ref[:, D + p * 128:D + (p + 1) * 128])
        oc_s[here, cols] = pick_heads(o2, TILE).astype(BF)
    x2 = (x1.astype(F32) + dnn(oc_s[here, :], wco[0])).astype(BF).astype(F32)

    normed2, rstd2 = layer_norm(x2)
    n_s[here, :] = (normed2 * (1.0 + mod(4)) + mod(3)).astype(BF)
    m_ref[...] = jnp.zeros_like(m_ref)

    if not backward:
        def mlp_fwd(c, carry):
            cols = pl.ds(pl.multiple_of(c * CH, CH), CH)
            u = dnn(n_s[here, :], win[0, :, cols])
            hid = (0.5 * u * (1.0 + jnp.tanh(K0 * (u + K1 * u * u * u)))).astype(BF)
            m_ref[...] += dnn(hid, wmo[0, cols, :])
            return carry

        lax.fori_loop(0, HID // CH, mlp_fwd, 0)
        x3 = x2 + mod(5) * m_ref[...]
        for f in range(4):
            for j in range(4):
                lo = f * 96 + j * 24
                out_ref[j, 0, f] = x3[lo:lo + 24].astype(BF)
        return

    def load_g():
        if temporal:
            return dnn(perm_ref[...], g_ref[...].reshape(TILE, D))
        return jnp.concatenate([g_ref[j, 0, f].astype(F32) for f in range(4) for j in range(4)], axis=0)

    g = load_g()
    dm_s[here, :] = (mod(5) * g).astype(BF)
    dn_ref[...] = jnp.zeros_like(dn_ref)

    def mlp_both(c, carry):
        cols = pl.ds(pl.multiple_of(c * CH, CH), CH)
        u = dnn(n_s[here, :], win[0, :, cols])
        u2 = u * u
        th = jnp.tanh(K0 * (u + K1 * u * u2))
        half = 0.5 * (1.0 + th)
        hid = (u * half).astype(BF)
        hid_s[here, cols] = hid
        slope = half + 0.5 * K0 * u * (1.0 - th * th) * (1.0 + 3.0 * K1 * u2)
        m_ref[...] += dnn(hid, wmo[0, cols, :])
        du = (dnt(dm_s[here, :], wmo[0, cols, :]) * slope).astype(BF)
        du_s[here, cols] = du
        dn_ref[...] += dnt(du, win[0, :, cols])
        return carry

    lax.fori_loop(0, HID // CH, mlp_both, 0)

    def add_mod(index, value):
        acc_ref[R_MOD + 8 * index:R_MOD + 8 * index + 8, :] += rows8(value)

    add_mod(5, g * m_ref[...])
    dn = dn_ref[...]
    add_mod(3, dn)
    add_mod(4, dn * normed2)
    dx2 = (g + layer_norm_bwd(dn * (1.0 + mod(4)), normed2, rstd2)).astype(BF)
    dx2_s[here, :] = dx2

    do_ref[...] = dnt(dx2, wco[0]).astype(BF)
    for p in range(3):
        cols = slice(p * 128, (p + 1) * 128)
        vcols = slice(D + p * 128, D + (p + 1) * 128)
        q2 = stack_heads(dqc_s[here, cols], low, high)
        do2 = stack_heads(do_ref[:, cols], low, high)
        prob = pc_ref[p]
        dp = dnt(do2, kv_ref[:, vcols])
        ds = (prob * (dp - jnp.sum(prob * dp, axis=-1, keepdims=True)) * 0.125).astype(BF)
        dqc_s[here, cols] = pick_heads(dnn(ds, kv_ref[:, cols]), TILE).astype(BF)
        dkv_ref[:, cols] += dtn(ds, q2)
        dkv_ref[:, vcols] += dtn(prob.astype(BF), do2)
    dx1 = (dx2.astype(F32) + dnn(dqc_s[here, :], wcq[0])).astype(BF)
    dx1f = dx1.astype(F32)

    add_mod(2, dx1f * a_ref[...])
    da = (mod(2) * dx1f).astype(BF)
    da_s[here, :] = da
    do_ref[...] = dnt(da, wout[0]).astype(BF)

    def self_bwd(grp, carry):
        rows = pl.ds(pl.multiple_of(grp * GRP, GRP), GRP)
        for p in range(3):
            cols = slice(p * 128, (p + 1) * 128)
            kcols = slice(D + p * 128, D + (p + 1) * 128)
            q2 = stack_heads(qb_ref[rows, cols], low, high)
            do2 = stack_heads(do_ref[rows, cols], low, high)
            prob = ps_ref[grp * 3 + p]
            dp = dnt(do2, vb_ref[rows, cols])
            ds = (prob * (dp - jnp.sum(prob * dp, axis=-1, keepdims=True)) * 0.125).astype(BF)
            dqk_ref[rows, cols] = pick_heads(dnn(ds, qb_ref[rows, kcols]), GRP)
            dqk_ref[rows, kcols] = dtn(ds, q2)
            dqkv_s[pl.ds(pl.multiple_of(r0 + grp * GRP, GRP), GRP), 2 * D + p * 128:2 * D + (p + 1) * 128] = dtn(prob.astype(BF), do2).astype(BF)
        return carry

    lax.fori_loop(0, NG, self_bwd, 0)
    for j in range(6):
        cols = slice(j * 128, (j + 1) * 128)
        grad = dqk_ref[:, cols]
        if temporal:
            grad = grad * cos_ref[...] - swap_halves(grad) * sin_ref[...]
        unit = qn_ref[:, cols]
        mean = head_sum(grad * unit, ones) * (1.0 / 64)
        dqkv_s[here, cols] = (rq_ref[:, cols] * (grad - unit * mean)).astype(BF)
    dh = dnn(dqkv_s[here, :], wqkv[0])
    normed, rstd = layer_norm(load_x())
    add_mod(0, dh)
    add_mod(1, dh * normed)
    dx = dx1f + layer_norm_bwd(dh * (1.0 + mod(1)), normed, rstd)
    if temporal:
        back = dtn(perm_ref[...], dx.astype(BF))
        out_ref[...] = back.astype(BF).reshape(4, 1, 12, 8, D)
    else:
        out_ref[...] = dx.astype(BF).reshape(1, 4, 96, D)

    @pl.when(t == TILES - 1)
    def _():
        acc_ref[R_OUT:R_CQ, :] += dtn(o_s[...], da_s[...])
        acc_ref[R_CQ:R_CKV, :] += dtn(dqc_s[...], x1_s[...])
        acc_ref[R_CKV:R_CO, :] += dtn(dkv_ref[...].astype(BF), cap_ref[0])
        acc_ref[R_CO:R_MO, :] += dtn(oc_s[...], dx2_s[...])

        def qkv_rows(c, carry):
            rows = pl.ds(pl.multiple_of(R_QKV + c * D, 128), D)
            acc_ref[rows, :] += dtn(dqkv_s[:, pl.ds(pl.multiple_of(c * D, 128), D)], h_s[...])
            return carry

        lax.fori_loop(0, 3, qkv_rows, 0)

        def mlp_rows(c, carry):
            cols = pl.ds(pl.multiple_of(c * 512, 512), 512)
            acc_ref[pl.ds(pl.multiple_of(R_MO + c * 512, 512), 512), :] += dtn(hid_s[:, cols], dm_s[...])
            accw_ref[:, cols] += dtn(n_s[...], du_s[:, cols])
            return carry

        lax.fori_loop(0, 3, mlp_rows, 0)


def run_block(index, temporal, backward, x, g, shared):
    mods, msk, cap, lens, weights, tables = shared
    samples = cap.shape[0]
    spatial_block = pl.BlockSpec((1, 4, 96, D), lambda s, t: (s, t, 0, 0))
    split_block = pl.BlockSpec((4, 1, 4, 24, D), lambda s, t: (0, s, t, 0, 0))
    cols_block = pl.BlockSpec((4, 1, 12, 8, D), lambda s, t: (0, s, 0, t, 0))

    def const(shape, first=0):
        return pl.BlockSpec(shape, lambda s, t: (first,) + (0,) * (len(shape) - 1), pipeline_mode=pl.Buffered(1))

    in_specs = [pl.BlockSpec(memory_space=pltpu.SMEM), cols_block if temporal else spatial_block]
    operands = [lens, x]
    if backward:
        in_specs.append(cols_block if temporal else split_block)
        operands.append(g)
    in_specs += [
        pl.BlockSpec((1, 16, D), lambda s, t: (s, 0, 0)),
        pl.BlockSpec((1, 1, TILE, 1), lambda s, t: (s, t, 0, 0)),
        pl.BlockSpec((1, CAP, D), lambda s, t: (s, 0, 0)),
    ]
    operands += [mods, msk, cap]
    for weight in weights:
        in_specs.append(const((1,) + weight.shape[1:], index))
        operands.append(weight)
    if temporal:
        for table in tables:
            in_specs.append(const(table.shape))
            operands.append(table)

    def vm(rows, cols, dtype=BF):
        return pltpu.VMEM((rows, cols), dtype)

    keep = ROWS if backward else TILE
    scratch = [vm(TILE, 2 * D), vm(TILE, D), vm(CAP, 2 * D), vm(TILE, D, F32)] + [vm(keep, D)] * 5
    split_shape = jax.ShapeDtypeStruct((4, samples, 12, 24, D), BF)
    if backward:
        out_shape = [
            split_shape if temporal else jax.ShapeDtypeStruct((samples, 12, 96, D), BF),
            jax.ShapeDtypeStruct((R_END, D), F32),
            jax.ShapeDtypeStruct((D, HID), F32),
        ]
        out_specs = [
            cols_block if temporal else spatial_block,
            pl.BlockSpec((R_END, D), lambda s, t: (0, 0), pipeline_mode=pl.Buffered(1)),
            pl.BlockSpec((D, HID), lambda s, t: (0, 0), pipeline_mode=pl.Buffered(1)),
        ]
        scratch += [vm(ROWS, HID), vm(ROWS, D), vm(ROWS, HID), vm(ROWS, D), vm(ROWS, D), vm(ROWS, D), vm(ROWS, 3 * D)]
        scratch += [
            vm(TILE, 2 * D, F32), vm(TILE, 2 * D, F32),
            pltpu.VMEM((3 * NG, 2 * GRP, GRP), F32), pltpu.VMEM((3, 2 * TILE, CAP), F32),
            vm(TILE, D, F32), vm(TILE, D, F32), vm(CAP, 2 * D, F32), vm(TILE, D), vm(TILE, 2 * D, F32),
        ]
    else:
        out_shape = split_shape
        out_specs = split_block
    flops = samples * ROWS * (13 if backward else 4.6) * 1e6
    return pl.pallas_call(
        functools.partial(block_kernel, temporal, backward),
        grid=(samples, TILES),
        in_specs=in_specs,
        out_specs=out_specs,
        out_shape=out_shape,
        scratch_shapes=scratch,
        compiler_params=pltpu.CompilerParams(
            dimension_semantics=("arbitrary", "arbitrary"), vmem_limit_bytes=VMEM_LIMIT),
        cost_estimate=pl.CostEstimate(flops=int(flops), bytes_accessed=20_000_000, transcendentals=0),
        name=("temporal" if temporal else "spatial") + ("_bwd" if backward else "_fwd"),
    )(*operands)


def rotary_tables():
    row_frame = jnp.arange(TILE) % 48
    inv_freq = 10000.0 ** (-jnp.arange(32, dtype=F32) / 32)
    angle = row_frame.astype(F32)[:, None] * inv_freq[None, :]
    cosine = jnp.tile(jnp.cos(angle), (1, 4))
    sine = jnp.sin(angle)
    signed = jnp.tile(jnp.concatenate([-sine, sine], axis=1), (1, 2))
    source = (jnp.arange(TILE) % 48) * 8 + jnp.arange(TILE) // 48
    perm = (source[:, None] == jnp.arange(TILE)[None, :]).astype(BF)
    return cosine, signed, perm


def solution(mesh):
    tok_spec = P('dp', 'sp')
    row_spec = P('dp')
    in_specs = (tok_spec, row_spec, row_spec, row_spec, row_spec, row_spec, P(), P(), P(), P(), P(), P(), P(), P(), tok_spec)
    out_specs = (tok_spec, P(), P(), P(), P(), P(), P(), P(), P())

    def local_step(latents, t_mod, t_mod_zero, frame_mask, captions, caption_len, w_qkv, w_out, w_cross_q, w_cross_kv, w_cross_out, w_mlp_in, w_mlp_out, mod_table, grad_out):
        samples = latents.shape[0]
        exchange = functools.partial(lax.all_to_all, axis_name='sp', split_axis=0, concat_axis=0, tiled=True)
        grad_split = jnp.moveaxis(grad_out.reshape(samples, 12, 4, 24, D), 2, 0)
        grad_cols = exchange(grad_split)
        weights = (
            jnp.transpose(w_qkv, (0, 2, 3, 4, 1)).reshape(2, 3 * D, D),
            w_out.reshape(2, D, D),
            jnp.transpose(w_cross_q, (0, 2, 3, 1)).reshape(2, D, D),
            jnp.transpose(w_cross_kv, (0, 2, 3, 4, 1)).reshape(2, 2 * D, D),
            w_cross_out.reshape(2, D, D),
            w_mlp_in,
            w_mlp_out,
        )
        cap = jnp.pad(captions, ((0, 0), (0, CAP - captions.shape[1]), (0, 0)))
        pad2 = ((0, 0), (0, 2), (0, 0))

        def mods_of(index):
            return jnp.concatenate([jnp.pad(mod_table[index] + t_mod, pad2), jnp.pad(mod_table[index] + t_mod_zero, pad2)], axis=1)

        mask = frame_mask.astype(F32)
        local_mask = lax.dynamic_slice_in_dim(mask, lax.axis_index('sp') * 12, 12, axis=1)
        msk_rows = jnp.repeat(local_mask, 96, axis=1).reshape(samples, TILES, TILE, 1)
        msk_cols = jnp.tile(mask, (1, 24)).reshape(samples, TILES, TILE, 1)
        tables = rotary_tables()
        shared0 = (mods_of(0), msk_rows, cap, caption_len, weights, tables)
        shared1 = (mods_of(1), msk_cols, cap, caption_len, weights, tables)

        middle = run_block(0, False, False, latents, None, shared0)
        dmid, acc1, accw1 = run_block(1, True, True, exchange(middle), grad_cols, shared1)
        sum1 = lax.psum((acc1, accw1), ('dp', 'sp'))
        grad_latents, acc0, accw0 = run_block(0, False, True, latents, exchange(dmid), shared0)
        acc0, accw0, sum1 = lax.optimization_barrier((acc0, accw0, sum1))
        sum0 = lax.psum((acc0, accw0), ('dp', 'sp'))

        def rows(first, last):
            return jnp.stack([sum0[0][first:last], sum1[0][first:last]])

        g_qkv = jnp.transpose(rows(R_QKV, R_OUT).reshape(2, 3, 6, 64, D), (0, 4, 1, 2, 3))
        g_out = rows(R_OUT, R_CQ).reshape(2, 6, 64, D)
        g_cq = jnp.transpose(rows(R_CQ, R_CKV).reshape(2, 6, 64, D), (0, 3, 1, 2))
        g_ckv = jnp.transpose(rows(R_CKV, R_CO).reshape(2, 2, 6, 64, D), (0, 4, 1, 2, 3))
        g_co = rows(R_CO, R_MO).reshape(2, 6, 64, D)
        g_mo = rows(R_MO, R_MOD)
        g_mi = jnp.stack([sum0[1], sum1[1]])
        g_mod = jnp.sum(rows(R_MOD, R_END).reshape(2, 6, 8, D), axis=2)
        return grad_latents, g_qkv, g_out, g_cq, g_ckv, g_co, g_mi, g_mo, g_mod

    return jax.shard_map(local_step, mesh=mesh, in_specs=in_specs, out_specs=out_specs, check_vma=False)
```

```python
import functools

import jax
import jax.numpy as jnp
from jax import lax
from jax.experimental import pallas as pl
from jax.experimental.pallas import tpu as pltpu
from jax.sharding import PartitionSpec as P

BF = jnp.bfloat16
F32 = jnp.float32
D = 384
HID = 1536
TILE = 384
GRP = 96
NG = TILE // GRP
TILES = 3
ROWS = TILE * TILES
CAP = 128
CH = 512
K0 = 0.7978845608028654
K1 = 0.044715
R_QKV, R_OUT, R_CQ, R_CKV, R_CO, R_MO, R_MOD, R_END = 0, 1152, 1536, 1920, 2688, 3072, 4608, 4656
VMEM_LIMIT = 66 * 1000 * 1000


def dnn(a, b):
    return lax.dot_general(a, b, (((1,), (0,)), ((), ())), preferred_element_type=F32)


def dnt(a, b):
    return lax.dot_general(a, b, (((1,), (1,)), ((), ())), preferred_element_type=F32)


def dtn(a, b):
    return lax.dot_general(a, b, (((0,), (0,)), ((), ())), preferred_element_type=F32)


def layer_norm(x):
    centered = x - jnp.mean(x, axis=-1, keepdims=True)
    rstd = lax.rsqrt(jnp.mean(centered * centered, axis=-1, keepdims=True) + 1e-6)
    return centered * rstd, rstd


def layer_norm_bwd(grad, normed, rstd):
    mean_g = jnp.mean(grad, axis=-1, keepdims=True)
    mean_gn = jnp.mean(grad * normed, axis=-1, keepdims=True)
    return rstd * (grad - mean_g - normed * mean_gn)


def rows8(x):
    return jnp.sum(x.reshape(x.shape[0] // 8, 8, x.shape[1]), axis=0)


def lane_low(rows):
    return lax.broadcasted_iota(jnp.int32, (rows, 128), 1) < 64


def head_sum_matrix():
    row = lax.broadcasted_iota(jnp.int32, (256, 128), 0)
    col = lax.broadcasted_iota(jnp.int32, (256, 128), 1)
    return jnp.where((row % 128) // 64 == col // 64, 1.0, 0.0).astype(BF)


def head_sum(x, ones):
    hi = x.astype(BF)
    lo = (x - hi.astype(F32)).astype(BF)
    return dnn(jnp.concatenate([hi, lo], axis=1), ones)


def swap_halves(x):
    lane = lax.broadcasted_iota(jnp.int32, x.shape, 1)
    return jnp.where(lane % 64 < 32, pltpu.roll(x, 96, 1), pltpu.roll(x, 32, 1))


def stack_heads(x, low, high):
    return jnp.concatenate([x * low, x * high], axis=0)


def pick_heads(x2, rows):
    return jnp.where(lane_low(rows), x2[:rows], x2[rows:])


def block_kernel(temporal, backward, first, chained, len_ref, *refs):
    refs = list(refs)
    take = refs.pop
    x_ref = take(0)
    g_ref = take(0) if backward else None
    mods_ref, msk_ref, cap_ref = take(0), take(0), take(0)
    wqkv, wout, wcq, wckv, wco, win, wmo = [take(0) for _ in range(7)]
    if temporal:
        cos_ref, sin_ref, perm_ref = take(0), take(0), take(0)
    if chained:
        acc_in, accw_in = take(0), take(0)
    out_ref = take(0)
    if backward:
        acc_ref, accw_ref = take(0), take(0)
    qb_ref, vb_ref, kv_ref, m_ref = take(0), take(0), take(0), take(0)
    h_s, o_s, x1_s, oc_s, n_s = [take(0) for _ in range(5)]
    if backward:
        hid_s, dm_s, du_s, dx2_s, dqc_s, da_s, dqkv_s = [take(0) for _ in range(7)]
        qn_ref, rq_ref, ps_ref, pc_ref, a_ref, dn_ref, dkv_ref, do_ref, dqk_ref = [take(0) for _ in range(9)]

    s = pl.program_id(0)
    t = pl.program_id(1)
    r0 = pl.multiple_of(t * TILE, TILE) if backward else 0
    here = pl.ds(r0, TILE)
    lane_row = lax.broadcasted_iota(jnp.int32, (1, 128), 1)
    low = jnp.where(lane_row < 64, 1.0, 0.0).astype(BF)
    high = jnp.where(lane_row < 64, 0.0, 1.0).astype(BF)
    ones = head_sum_matrix()
    cond = msk_ref[0, 0] > 0.5

    def mod(index):
        return jnp.where(cond, mods_ref[0, index:index + 1, :], mods_ref[0, 8 + index:9 + index, :])

    if backward:
        @pl.when((s == 0) & (t == 0))
        def _():
            if chained:
                pltpu.sync_copy(acc_in, acc_ref)
                pltpu.sync_copy(accw_in, accw_ref)
            else:
                acc_ref[...] = jnp.zeros_like(acc_ref)
                accw_ref[...] = jnp.zeros_like(accw_ref)

    @pl.when(t == 0)
    def _():
        kv_ref[...] = dnt(cap_ref[0], wckv[0]).astype(BF)
        if backward:
            dkv_ref[...] = jnp.zeros_like(dkv_ref)

    def load_x():
        if temporal:
            return dnn(perm_ref[...], x_ref[...].reshape(TILE, D))
        return x_ref[...].reshape(TILE, D).astype(F32)

    normed, _ = layer_norm(load_x())
    h = (normed * (1.0 + mod(1)) + mod(0)).astype(BF)
    h_s[here, :] = h
    qkv = dnt(h, wqkv[0])
    for j in range(6):
        cols = slice(j * 128, (j + 1) * 128)
        raw = qkv[:, cols]
        inv = lax.rsqrt(head_sum(raw * raw, ones) * (1.0 / 64) + 1e-6)
        unit = raw * inv
        if backward:
            qn_ref[:, cols] = unit
            rq_ref[:, cols] = inv
        if temporal:
            unit = unit * cos_ref[...] + swap_halves(unit) * sin_ref[...]
        qb_ref[:, cols] = unit.astype(BF)
    vb_ref[...] = qkv[:, 2 * D:].astype(BF)

    if temporal:
        same = (lax.broadcasted_iota(jnp.int32, (2 * GRP, GRP), 0) // 48) % 2 == lax.broadcasted_iota(jnp.int32, (2 * GRP, GRP), 1) // 48

    def self_fwd(grp, carry):
        rows = pl.ds(pl.multiple_of(grp * GRP, GRP), GRP)
        for p in range(3):
            cols = slice(p * 128, (p + 1) * 128)
            kcols = slice(D + p * 128, D + (p + 1) * 128)
            q2 = stack_heads(qb_ref[rows, cols], low, high)
            e = jnp.exp(dnt(q2, qb_ref[rows, kcols]) * 0.125)
            if temporal:
                e = jnp.where(same, e, 0.0)
            prob = e * (1.0 / jnp.sum(e, axis=-1, keepdims=True))
            if backward:
                ps_ref[grp * 3 + p] = prob
            o2 = dnn(prob.astype(BF), vb_ref[rows, cols])
            o_s[pl.ds(pl.multiple_of(r0 + grp * GRP, GRP), GRP), cols] = pick_heads(o2, GRP).astype(BF)
        return carry

    lax.fori_loop(0, NG, self_fwd, 0, unroll=True)

    attn = dnn(o_s[here, :], wout[0])
    if backward:
        a_ref[...] = attn
    x1 = (load_x() + mod(2) * attn).astype(BF)
    x1_s[here, :] = x1

    qc = dnt(x1, wcq[0]).astype(BF)
    valid = lax.broadcasted_iota(jnp.int32, (2 * TILE, CAP), 1) < len_ref[s + first]
    for p in range(3):
        cols = slice(p * 128, (p + 1) * 128)
        q2 = stack_heads(qc[:, cols], low, high)
        sc = jnp.where(valid, dnt(q2, kv_ref[:, cols]) * 0.125, -1e30)
        e = jnp.exp(sc - jnp.max(sc, axis=-1, keepdims=True))
        prob = e * (1.0 / jnp.sum(e, axis=-1, keepdims=True))
        if backward:
            pc_ref[p] = prob
            dqc_s[here, cols] = qc[:, cols]
        o2 = dnn(prob.astype(BF), kv_ref[:, D + p * 128:D + (p + 1) * 128])
        oc_s[here, cols] = pick_heads(o2, TILE).astype(BF)
    x2 = (x1.astype(F32) + dnn(oc_s[here, :], wco[0])).astype(BF).astype(F32)

    normed2, rstd2 = layer_norm(x2)
    n_s[here, :] = (normed2 * (1.0 + mod(4)) + mod(3)).astype(BF)
    m_ref[...] = jnp.zeros_like(m_ref)

    if not backward:
        def mlp_fwd(c, carry):
            cols = pl.ds(pl.multiple_of(c * CH, CH), CH)
            u = dnn(n_s[here, :], win[0, :, cols])
            hid = (0.5 * u * (1.0 + jnp.tanh(K0 * (u + K1 * u * u * u)))).astype(BF)
            m_ref[...] += dnn(hid, wmo[0, cols, :])
            return carry

        lax.fori_loop(0, HID // CH, mlp_fwd, 0, unroll=True)
        x3 = x2 + mod(5) * m_ref[...]
        for f in range(4):
            for j in range(4):
                lo = f * 96 + j * 24
                out_ref[j, 0, f] = x3[lo:lo + 24].astype(BF)
        return

    def load_g():
        if temporal:
            return dnn(perm_ref[...], g_ref[...].reshape(TILE, D))
        return jnp.concatenate([g_ref[j, 0, f].astype(F32) for f in range(4) for j in range(4)], axis=0)

    g = load_g()
    dm_s[here, :] = (mod(5) * g).astype(BF)
    dn_ref[...] = jnp.zeros_like(dn_ref)

    def mlp_both(c, carry):
        cols = pl.ds(pl.multiple_of(c * CH, CH), CH)
        u = dnn(n_s[here, :], win[0, :, cols])
        u2 = u * u
        th = jnp.tanh(K0 * (u + K1 * u * u2))
        half = 0.5 * (1.0 + th)
        hid = (u * half).astype(BF)
        hid_s[here, cols] = hid
        slope = half + 0.5 * K0 * u * (1.0 - th * th) * (1.0 + 3.0 * K1 * u2)
        m_ref[...] += dnn(hid, wmo[0, cols, :])
        du = (dnt(dm_s[here, :], wmo[0, cols, :]) * slope).astype(BF)
        du_s[here, cols] = du
        dn_ref[...] += dnt(du, win[0, :, cols])
        return carry

    lax.fori_loop(0, HID // CH, mlp_both, 0, unroll=True)

    def add_mod(index, value):
        acc_ref[R_MOD + 8 * index:R_MOD + 8 * index + 8, :] += rows8(value)

    add_mod(5, g * m_ref[...])
    dn = dn_ref[...]
    add_mod(3, dn)
    add_mod(4, dn * normed2)
    dx2 = (g + layer_norm_bwd(dn * (1.0 + mod(4)), normed2, rstd2)).astype(BF)
    dx2_s[here, :] = dx2

    do_ref[...] = dnt(dx2, wco[0]).astype(BF)
    for p in range(3):
        cols = slice(p * 128, (p + 1) * 128)
        vcols = slice(D + p * 128, D + (p + 1) * 128)
        q2 = stack_heads(dqc_s[here, cols], low, high)
        do2 = stack_heads(do_ref[:, cols], low, high)
        prob = pc_ref[p]
        dp = dnt(do2, kv_ref[:, vcols])
        ds = (prob * (dp - jnp.sum(prob * dp, axis=-1, keepdims=True)) * 0.125).astype(BF)
        dqc_s[here, cols] = pick_heads(dnn(ds, kv_ref[:, cols]), TILE).astype(BF)
        dkv_ref[:, cols] += dtn(ds, q2)
        dkv_ref[:, vcols] += dtn(prob.astype(BF), do2)
    dx1 = (dx2.astype(F32) + dnn(dqc_s[here, :], wcq[0])).astype(BF)
    dx1f = dx1.astype(F32)

    add_mod(2, dx1f * a_ref[...])
    da = (mod(2) * dx1f).astype(BF)
    da_s[here, :] = da
    do_ref[...] = dnt(da, wout[0]).astype(BF)

    def self_bwd(grp, carry):
        rows = pl.ds(pl.multiple_of(grp * GRP, GRP), GRP)
        for p in range(3):
            cols = slice(p * 128, (p + 1) * 128)
            kcols = slice(D + p * 128, D + (p + 1) * 128)
            q2 = stack_heads(qb_ref[rows, cols], low, high)
            do2 = stack_heads(do_ref[rows, cols], low, high)
            prob = ps_ref[grp * 3 + p]
            dp = dnt(do2, vb_ref[rows, cols])
            ds = (prob * (dp - jnp.sum(prob * dp, axis=-1, keepdims=True)) * 0.125).astype(BF)
            dqk_ref[rows, cols] = pick_heads(dnn(ds, qb_ref[rows, kcols]), GRP)
            dqk_ref[rows, kcols] = dtn(ds, q2)
            dqkv_s[pl.ds(pl.multiple_of(r0 + grp * GRP, GRP), GRP), 2 * D + p * 128:2 * D + (p + 1) * 128] = dtn(prob.astype(BF), do2).astype(BF)
        return carry

    lax.fori_loop(0, NG, self_bwd, 0, unroll=True)
    for j in range(6):
        cols = slice(j * 128, (j + 1) * 128)
        grad = dqk_ref[:, cols]
        if temporal:
            grad = grad * cos_ref[...] - swap_halves(grad) * sin_ref[...]
        unit = qn_ref[:, cols]
        mean = head_sum(grad * unit, ones) * (1.0 / 64)
        dqkv_s[here, cols] = (rq_ref[:, cols] * (grad - unit * mean)).astype(BF)
    dh = dnn(dqkv_s[here, :], wqkv[0])
    normed, rstd = layer_norm(load_x())
    add_mod(0, dh)
    add_mod(1, dh * normed)
    dx = dx1f + layer_norm_bwd(dh * (1.0 + mod(1)), normed, rstd)
    if temporal:
        back = dtn(perm_ref[...], dx.astype(BF))
        out_ref[...] = back.astype(BF).reshape(4, 1, 12, 8, D)
    else:
        out_ref[...] = dx.astype(BF).reshape(1, 4, 96, D)

    @pl.when(t == TILES - 1)
    def _():
        acc_ref[R_OUT:R_CQ, :] += dtn(o_s[...], da_s[...])
        acc_ref[R_CQ:R_CKV, :] += dtn(dqc_s[...], x1_s[...])
        acc_ref[R_CKV:R_CO, :] += dtn(dkv_ref[...].astype(BF), cap_ref[0])
        acc_ref[R_CO:R_MO, :] += dtn(oc_s[...], dx2_s[...])

        def qkv_rows(c, carry):
            rows = pl.ds(pl.multiple_of(R_QKV + c * D, 128), D)
            acc_ref[rows, :] += dtn(dqkv_s[:, pl.ds(pl.multiple_of(c * D, 128), D)], h_s[...])
            return carry

        lax.fori_loop(0, 3, qkv_rows, 0)

        def mlp_rows(c, carry):
            cols = pl.ds(pl.multiple_of(c * 512, 512), 512)
            acc_ref[pl.ds(pl.multiple_of(R_MO + c * 512, 512), 512), :] += dtn(hid_s[:, cols], dm_s[...])
            accw_ref[:, cols] += dtn(n_s[...], du_s[:, cols])
            return carry

        lax.fori_loop(0, 3, mlp_rows, 0)


def run_block(index, temporal, backward, x, g, shared, first, samples, acc=None):
    mods, msk, cap, lens, weights, tables = shared
    spatial_in = pl.BlockSpec((1, 4, 96, D), lambda s, t: (s + first, t, 0, 0))
    spatial_block = pl.BlockSpec((1, 4, 96, D), lambda s, t: (s, t, 0, 0))
    split_block = pl.BlockSpec((4, 1, 4, 24, D), lambda s, t: (0, s, t, 0, 0))
    cols_block = pl.BlockSpec((4, 1, 12, 8, D), lambda s, t: (0, s, 0, t, 0))
    cols_whole = pl.BlockSpec((4, 1, 12, 8, D), lambda s, t: (0, s + first, 0, t, 0))

    def const(shape, lead=0):
        return pl.BlockSpec(shape, lambda s, t: (lead,) + (0,) * (len(shape) - 1), pipeline_mode=pl.Buffered(1))

    in_specs = [pl.BlockSpec(memory_space=pltpu.SMEM), cols_block if temporal else spatial_in]
    operands = [lens, x]
    if backward:
        in_specs.append(cols_whole if temporal else split_block)
        operands.append(g)
    in_specs += [
        pl.BlockSpec((1, 16, D), lambda s, t: (s + first, 0, 0)),
        pl.BlockSpec((1, 1, TILE, 1), lambda s, t: (s + first, t, 0, 0)),
        pl.BlockSpec((1, CAP, D), lambda s, t: (s + first, 0, 0)),
    ]
    operands += [mods, msk, cap]
    for weight in weights:
        in_specs.append(const((1,) + weight.shape[1:], index))
        operands.append(weight)
    if temporal:
        for table in tables:
            in_specs.append(const(table.shape))
            operands.append(table)
    if acc is not None:
        in_specs += [pl.BlockSpec(memory_space=pl.ANY)] * 2
        operands += list(acc)

    def vm(rows, cols, dtype=BF):
        return pltpu.VMEM((rows, cols), dtype)

    keep = ROWS if backward else TILE
    scratch = [vm(TILE, 2 * D), vm(TILE, D), vm(CAP, 2 * D), vm(TILE, D, F32)] + [vm(keep, D)] * 5
    split_shape = jax.ShapeDtypeStruct((4, samples, 12, 24, D), BF)
    if backward:
        out_shape = [
            split_shape if temporal else jax.ShapeDtypeStruct((samples, 12, 96, D), BF),
            jax.ShapeDtypeStruct((R_END, D), F32),
            jax.ShapeDtypeStruct((D, HID), F32),
        ]
        out_specs = [
            cols_block if temporal else spatial_block,
            pl.BlockSpec((R_END, D), lambda s, t: (0, 0), pipeline_mode=pl.Buffered(1)),
            pl.BlockSpec((D, HID), lambda s, t: (0, 0), pipeline_mode=pl.Buffered(1)),
        ]
        scratch += [vm(ROWS, HID), vm(ROWS, D), vm(ROWS, HID), vm(ROWS, D), vm(ROWS, D), vm(ROWS, D), vm(ROWS, 3 * D)]
        scratch += [
            vm(TILE, 2 * D, F32), vm(TILE, 2 * D, F32),
            pltpu.VMEM((3 * NG, 2 * GRP, GRP), F32), pltpu.VMEM((3, 2 * TILE, CAP), F32),
            vm(TILE, D, F32), vm(TILE, D, F32), vm(CAP, 2 * D, F32), vm(TILE, D), vm(TILE, 2 * D, F32),
        ]
    else:
        out_shape = split_shape
        out_specs = split_block
    flops = samples * ROWS * (13 if backward else 4.6) * 1e6
    return pl.pallas_call(
        functools.partial(block_kernel, temporal, backward, first, acc is not None),
        grid=(samples, TILES),
        in_specs=in_specs,
        out_specs=out_specs,
        out_shape=out_shape,
        scratch_shapes=scratch,
        compiler_params=pltpu.CompilerParams(
            dimension_semantics=("arbitrary", "arbitrary"), vmem_limit_bytes=VMEM_LIMIT),
        cost_estimate=pl.CostEstimate(flops=int(flops), bytes_accessed=20_000_000, transcendentals=0),
        name=("temporal" if temporal else "spatial") + ("_bwd" if backward else "_fwd"),
    )(*operands)


def rotary_tables():
    row_frame = jnp.arange(TILE) % 48
    inv_freq = 10000.0 ** (-jnp.arange(32, dtype=F32) / 32)
    angle = row_frame.astype(F32)[:, None] * inv_freq[None, :]
    cosine = jnp.tile(jnp.cos(angle), (1, 4))
    sine = jnp.sin(angle)
    signed = jnp.tile(jnp.concatenate([-sine, sine], axis=1), (1, 2))
    source = (jnp.arange(TILE) % 48) * 8 + jnp.arange(TILE) // 48
    perm = (source[:, None] == jnp.arange(TILE)[None, :]).astype(BF)
    return cosine, signed, perm


def solution(mesh):
    tok_spec = P('dp', 'sp')
    row_spec = P('dp')
    in_specs = (tok_spec, row_spec, row_spec, row_spec, row_spec, row_spec, P(), P(), P(), P(), P(), P(), P(), P(), tok_spec)
    out_specs = (tok_spec, P(), P(), P(), P(), P(), P(), P(), P())

    def local_step(latents, t_mod, t_mod_zero, frame_mask, captions, caption_len, w_qkv, w_out, w_cross_q, w_cross_kv, w_cross_out, w_mlp_in, w_mlp_out, mod_table, grad_out):
        samples = latents.shape[0]
        exchange = functools.partial(lax.all_to_all, axis_name='sp', split_axis=0, concat_axis=0, tiled=True)
        grad_split = jnp.moveaxis(grad_out.reshape(samples, 12, 4, 24, D), 2, 0)
        grad_cols = exchange(grad_split)
        weights = (
            jnp.transpose(w_qkv, (0, 2, 3, 4, 1)).reshape(2, 3 * D, D),
            w_out.reshape(2, D, D),
            jnp.transpose(w_cross_q, (0, 2, 3, 1)).reshape(2, D, D),
            jnp.transpose(w_cross_kv, (0, 2, 3, 4, 1)).reshape(2, 2 * D, D),
            w_cross_out.reshape(2, D, D),
            w_mlp_in,
            w_mlp_out,
        )
        cap = jnp.pad(captions, ((0, 0), (0, CAP - captions.shape[1]), (0, 0)))
        pad2 = ((0, 0), (0, 2), (0, 0))

        def mods_of(index):
            return jnp.concatenate([jnp.pad(mod_table[index] + t_mod, pad2), jnp.pad(mod_table[index] + t_mod_zero, pad2)], axis=1)

        mask = frame_mask.astype(F32)
        local_mask = lax.dynamic_slice_in_dim(mask, lax.axis_index('sp') * 12, 12, axis=1)
        msk_rows = jnp.repeat(local_mask, 96, axis=1).reshape(samples, TILES, TILE, 1)
        msk_cols = jnp.tile(mask, (1, 24)).reshape(samples, TILES, TILE, 1)
        tables = rotary_tables()
        shared0 = (mods_of(0), msk_rows, cap, caption_len, weights, tables)
        shared1 = (mods_of(1), msk_cols, cap, caption_len, weights, tables)

        cut = samples - 1
        middle_a = run_block(0, False, False, latents, None, shared0, 0, cut)
        late, grad_cols = lax.optimization_barrier((latents, grad_cols))
        middle_b = run_block(0, False, False, late, None, shared0, cut, 1)
        cols_a = exchange(middle_a)
        cols_b = exchange(middle_b)
        dmid_a, *acc1 = run_block(1, True, True, cols_a, grad_cols, shared1, 0, cut)
        dmid_b, *acc1 = run_block(1, True, True, cols_b, grad_cols, shared1, cut, 1, acc1)
        back_a = exchange(dmid_a)
        back_b = exchange(dmid_b)
        sum1 = lax.psum(tuple(acc1), ('dp', 'sp'))
        grad_a, *acc0 = run_block(0, False, True, latents, back_a, shared0, 0, cut)
        grad_b, acc0, accw0 = run_block(0, False, True, latents, back_b, shared0, cut, 1, acc0)
        grad_latents = jnp.concatenate([grad_a, grad_b], axis=0)
        acc0, accw0, sum1 = lax.optimization_barrier((acc0, accw0, sum1))
        sum0 = lax.psum((acc0, accw0), ('dp', 'sp'))

        def rows(first, last):
            return jnp.stack([sum0[0][first:last], sum1[0][first:last]])

        g_qkv = jnp.transpose(rows(R_QKV, R_OUT).reshape(2, 3, 6, 64, D), (0, 4, 1, 2, 3))
        g_out = rows(R_OUT, R_CQ).reshape(2, 6, 64, D)
        g_cq = jnp.transpose(rows(R_CQ, R_CKV).reshape(2, 6, 64, D), (0, 3, 1, 2))
        g_ckv = jnp.transpose(rows(R_CKV, R_CO).reshape(2, 2, 6, 64, D), (0, 4, 1, 2, 3))
        g_co = rows(R_CO, R_MO).reshape(2, 6, 64, D)
        g_mo = rows(R_MO, R_MOD)
        g_mi = jnp.stack([sum0[1], sum1[1]])
        g_mod = jnp.sum(rows(R_MOD, R_END).reshape(2, 6, 8, D), axis=2)
        return grad_latents, g_qkv, g_out, g_cq, g_ckv, g_co, g_mi, g_mo, g_mod

    return jax.shard_map(local_step, mesh=mesh, in_specs=in_specs, out_specs=out_specs, check_vma=False)
```
